32 devices in a mesh: row: 8 (over z, core), col: 4 (over y, x).
Axes of the slice: x: 2, y: 2, z: 4, core: 2. Of those that a mesh axis runs over, the one named last changes fastest.
Arguments:
- waves_row: bfloat16 [8, 64, 2048], P('row', None, 'col'), may hold values from -6 to 6
- waves_col: bfloat16 [4, 64, 2048], P('col', None, 'row'), may hold values from -6 to 6
- window_row: int32 [8], P('row'), may hold values from 0 to 32
- window_col: int32 [4], P('col'), may hold values from 0 to 32
- plane_wave: bfloat16 [2048, 1024], replicated, may hold values from -0.125 to 0.125
- screened: bfloat16 [8, 1024, 1024], P(None, 'row'), may hold values from -0.1875 to 0.1875
- owner_slot: int32 [8], replicated, may hold values from 0 to 7, each once
- transfer_table: int32 [8, 4], P(None, 'col'), may hold values from 0 to 7, as said below
- trial: bfloat16 [1024, 512], P('col'), may hold values from -6 to 6
Outputs:
- applied: float32 [2048, 512], P(('row', 'col'))
The draws below stay inside these ranges and needn't reach their ends.
Inputs may be any that keep to these rules, and one draw needn't show every extreme that they name: `transfer_table`: for every column k-point, the row k-points name each of the 8 momentum transfers exactly once.
All inputs are finite; a program needn't handle non-finite values.
Results may differ from the reference program's by a relative error of at most 0.014.
Values may be sent and summed in bfloat16 or wider, within the bound.
No kernel may reach another device: no remote copies, remote signals or barrier semaphores. Data moves between devices by JAX's collectives and lax.ppermute only.
A program may use at most 64 MiB of HBM per device.

```python
import jax
import jax.numpy as jnp
from jax import lax

NB = 64
NR = 2048
NG = 1024
NVW = 16
NCW = 16
NT = 512
NP = 256
NQ = 8
NKC = 4


def draw_transfer_table(key, part):
    first = jax.random.fold_in(key, 11)
    second = jax.random.fold_in(key, 23)
    row_labels = jax.random.permutation(first, NQ)
    col_labels = jax.random.permutation(second, NQ)[:NKC]
    return ((row_labels[:, None] - col_labels[None, :]) % NQ).astype(jnp.int32)


def plant(array, own_key, smallest, top_value):
    extent = array.shape
    place = [jax.random.randint(jax.random.fold_in(own_key, axis), (), 0, extent[axis]) for axis in range(len(extent))]
    array = array.at[tuple(place)].set(smallest)
    longest = extent.index(max(extent))
    place[longest] = (place[longest] + 1) % extent[longest]
    return array.at[tuple(place)].set(top_value)


def shard_levels(key, extent, cuts, least, largest):
    level, own = 1.0, jax.random.fold_in(key, 6)
    for dim, shards_of in cuts:
        draws = jnp.exp(jax.random.uniform(jax.random.fold_in(own, dim), (shards_of,), jnp.float32, least / len(cuts), largest / len(cuts)))
        level = level * jnp.repeat(draws, extent[dim] // shards_of).reshape([-1 if axis == dim else 1 for axis in range(len(extent))])
    return level


def noise(key, dims, scale, most, shards=(), kind=jnp.bfloat16):
    factor_of = shard_levels(key, dims, shards, -0.22, 0.18) if shards else 1.0
    result = jax.random.normal(key, dims, jnp.float32) * scale * factor_of
    return jnp.minimum(jnp.maximum(result, -most), most).astype(kind)


def setup_inputs(seed: int = 0) -> dict:
    keys = jax.random.split(jax.random.key(seed), 10)
    return {
        "waves_row": noise(keys[0], (NQ, NB, NR), 1.0, 6.0, ((0, 8), (2, 4))),
        "waves_col": noise(keys[1], (NKC, NB, NR), 1.0, 6.0, ((0, 4), (2, 8))),
        "window_row": plant(jax.random.randint(keys[2], (NQ,), 0, NB - NVW - NCW + 1), jax.random.fold_in(keys[2], 1), 0, NB - NVW - NCW).astype(jnp.int32),
        "window_col": plant(jax.random.randint(keys[3], (NKC,), 0, NB - NVW - NCW + 1), jax.random.fold_in(keys[3], 1), 0, NB - NVW - NCW).astype(jnp.int32),
        "plane_wave": noise(keys[4], (NR, NG), NR ** -0.5, 0.125),
        "screened": noise(keys[5], (NQ, NG, NG), NG ** -0.5, 0.1875, ((1, 8),)),
        "owner_slot": jax.random.permutation(keys[6], NQ).astype(jnp.int32),
        "transfer_table": draw_transfer_table(jax.random.fold_in(keys[9], 71), 0),
        "trial": noise(keys[8], (NKC * NP, NT), 1.0, 6.0, ((0, 4),)),
    }


def pair_products(waves, start):
    valence = lax.dynamic_slice_in_dim(waves, start, NVW, 0).astype(jnp.float32)
    conduction = lax.dynamic_slice_in_dim(waves, start + NVW, NCW, 0).astype(jnp.float32)
    return (valence[:, None, :] * conduction[None, :, :]).reshape(NVW * NCW, -1).astype(jnp.bfloat16)


def densities(waves, starts, plane_wave):
    def single(item):
        products = pair_products(item[0], item[1])
        return jnp.dot(products, plane_wave, preferred_element_type=jnp.float32).astype(jnp.bfloat16)
    return lax.map(single, (waves, starts))


def reference(waves_row, waves_col, window_row, window_col, plane_wave, screened, owner_slot, transfer_table, trial):
    dens_row = densities(waves_row, window_row, plane_wave)
    dens_col = densities(waves_col, window_col, plane_wave)
    trial_blocks = trial.reshape(NKC, NP, NT).astype(jnp.float32)
    scale = (NKC * NP) ** -0.5

    def one_row(item):
        dens, transfers = item
        chosen = screened[owner_slot[transfers]].astype(jnp.float32)
        weighted = jnp.einsum('jgh,jph->jgp', chosen, dens_col.astype(jnp.float32)).astype(jnp.bfloat16)
        block = jnp.einsum('pg,jgq->jpq', dens.astype(jnp.float32), weighted.astype(jnp.float32))
        block = (block * NG ** -0.5).astype(jnp.bfloat16)
        return jnp.einsum('jpq,jqt->pt', block.astype(jnp.float32), trial_blocks) * scale

    applied = lax.map(one_row, (dens_row, transfer_table))
    return applied.reshape(NQ * NP, NT)
```

```python
import functools

import jax
import jax.numpy as jnp
from jax import lax
from jax.experimental import pallas as pl
from jax.experimental.pallas import tpu as pltpu
from jax.sharding import PartitionSpec as P

NVW = 16
NCW = 16
NP = NVW * NCW
GRANT = 16 << 20
VMEM = pl.BlockSpec(memory_space=pltpu.VMEM)
SMEM = pl.BlockSpec(memory_space=pltpu.SMEM)


def call(kernel, outs, *args, scratch=(), flops=0, moved=0, scalars=0):
    return pl.pallas_call(
        kernel,
        out_shape=outs,
        in_specs=[SMEM] * scalars + [VMEM] * (len(args) - scalars),
        out_specs=jax.tree.map(lambda _: VMEM, outs),
        scratch_shapes=list(scratch),
        cost_estimate=pl.CostEstimate(flops=flops, bytes_accessed=moved, transcendentals=0),
        compiler_params=pltpu.CompilerParams(vmem_limit_bytes=GRANT),
    )(*args)


def density_kernel(count, place_ref, *refs):
    pieces, (table_ref, out_ref, prod_ref) = refs[:count], refs[count:]
    for step, piece in enumerate(pieces):
        points = piece.shape[1]
        bands = piece[...].astype(jnp.float32)
        valence, conduction = bands[:NVW], bands[NVW:]
        products = (valence[:, None, :] * conduction[None, :, :]).reshape(NP, points)
        at = pl.multiple_of(place_ref[step] * points, 128)
        prod_ref[:, pl.ds(at, points)] = products.astype(jnp.bfloat16)
    out_ref[...] = jnp.dot(
        prod_ref[...], table_ref[...], preferred_element_type=jnp.float32
    ).astype(jnp.bfloat16)


def density(places, pieces, table):
    points, waves = table.shape
    return call(
        functools.partial(density_kernel, len(pieces)),
        jax.ShapeDtypeStruct((NP, waves), jnp.bfloat16),
        places,
        *pieces,
        table,
        scratch=[pltpu.VMEM((NP, points), jnp.bfloat16)],
        flops=2 * NP * points * waves,
        moved=2 * points * waves,
        scalars=1,
    )


def weighted_kernel(slots_ref, screened_ref, dens_ref, out_ref):
    def body(k, carry):
        out_ref[k] = lax.dot_general(
            screened_ref[slots_ref[k]],
            dens_ref[...],
            (((1,), (1,)), ((), ())),
            preferred_element_type=jnp.float32,
        ).astype(jnp.bfloat16)
        return carry

    lax.fori_loop(0, out_ref.shape[0], body, 0)


def gather_cols(x, axis):
    n = lax.axis_size(axis)
    return [x] + [lax.ppermute(x, axis, [(i, i ^ s) for i in range(n)]) for s in range(1, n)]


def partial_kernel(count, place_ref, scale_block, scale, *refs):
    dens_ref, pieces, (trial_ref, out_ref) = refs[0], refs[1 : 1 + count], refs[1 + count :]
    total = None
    for step, piece in enumerate(pieces):
        rows = piece.shape[0]
        at = pl.multiple_of(place_ref[step] * rows, 128)
        term = jnp.dot(dens_ref[:, pl.ds(at, rows)], piece[...], preferred_element_type=jnp.float32)
        total = term if total is None else total + term
    block = (total * scale_block).astype(jnp.bfloat16)
    applied = jnp.dot(block, trial_ref[...], preferred_element_type=jnp.float32) * scale
    out_ref[...] = applied.astype(jnp.bfloat16)


def shards(
    waves_row,
    waves_col,
    window_row,
    window_col,
    plane_wave,
    screened,
    owner_slot,
    transfer_table,
    trial,
):
    rows, cols = lax.axis_size("row"), lax.axis_size("col")
    chips = rows // 2
    me_row, me_col = lax.axis_index("row"), lax.axis_index("col")
    waves = plane_wave.shape[1]
    share = screened.shape[1]

    bands_col = lax.dynamic_slice_in_dim(waves_col[0], window_col[0], NVW + NCW, 0)
    bands_row = lax.dynamic_slice_in_dim(waves_row[0], window_row[0], NVW + NCW, 0)
    other = lax.ppermute(bands_col, "row", [(i, i ^ 1) for i in range(rows)])
    even = me_row % 2 == 0
    pair = jnp.concatenate(
        [jnp.where(even, bands_col, other), jnp.where(even, other, bands_col)], axis=1
    )
    chip_pieces = [pair] + [
        lax.ppermute(pair, "row", [(i, i ^ (2 * s)) for i in range(rows)]) for s in range(1, chips)
    ]
    row_pieces = gather_cols(bands_row, "col")

    dens_col = density((me_row // 2) ^ jnp.arange(chips), chip_pieces, plane_wave)
    slots = owner_slot[transfer_table[:, 0]]
    weighted = call(
        weighted_kernel,
        jax.ShapeDtypeStruct((rows, share, NP), jnp.bfloat16),
        slots,
        screened,
        dens_col,
        flops=2 * rows * share * waves * NP,
        moved=2 * rows * share * waves,
        scalars=1,
    ).reshape(chips, 2 * share, NP)

    def message(s):
        return lax.dynamic_index_in_dim(weighted, (me_row // 2) ^ s, 0, keepdims=False)

    arrived = [message(0)] + [
        lax.ppermute(message(s), "row", [(i, i ^ (2 * s)) for i in range(rows)])
        for s in range(1, chips)
    ]
    stack = jnp.stack(arrived).reshape(chips, 2, share, NP)
    mine = lax.dynamic_index_in_dim(stack, me_row % 2, 1, keepdims=False)
    theirs = lax.dynamic_index_in_dim(stack, 1 - me_row % 2, 1, keepdims=False)
    theirs = lax.ppermute(theirs, "row", [(i, i ^ 1) for i in range(rows)])
    pieces = [mine[s] for s in range(chips)] + [theirs[s] for s in range(chips)]
    order = (me_row // 2) ^ jnp.arange(chips)
    places = jnp.concatenate([2 * order + me_row % 2, 2 * order + 1 - me_row % 2])

    dens_row = density(me_col ^ jnp.arange(cols), row_pieces, plane_wave)
    scale = (cols * NP) ** (-0.5)

    def kernel(place_ref, *refs):
        partial_kernel(len(pieces), place_ref, waves ** (-0.5), scale, *refs)

    partial = call(
        kernel,
        jax.ShapeDtypeStruct((NP, trial.shape[1]), jnp.bfloat16),
        places,
        dens_row,
        *pieces,
        trial,
        flops=2 * NP * waves * NP + 2 * NP * NP * trial.shape[1],
        moved=2 * NP * waves,
        scalars=1,
    ).reshape(cols, NP // cols, trial.shape[1])

    def part(s):
        return lax.dynamic_index_in_dim(partial, me_col ^ s, 0, keepdims=False)

    total = part(0).astype(jnp.float32)
    for s in range(1, cols):
        total += lax.ppermute(part(s), "col", [(i, i ^ s) for i in range(cols)]).astype(jnp.float32)
    return total


def solution(mesh):
    return jax.shard_map(
        shards,
        mesh=mesh,
        in_specs=(
            P("row", None, "col"),
            P("col", None, "row"),
            P("row"),
            P("col"),
            P(),
            P(None, "row", None),
            P(),
            P(None, "col"),
            P("col", None),
        ),
        out_specs=P(("row", "col"), None),
        check_vma=False,
    )
```

```python
import functools

import jax
import jax.numpy as jnp
from jax import lax
from jax.experimental import pallas as pl
from jax.experimental.pallas import tpu as pltpu
from jax.sharding import PartitionSpec as P


NVW = 16
NCW = 16
NP = NVW * NCW
GRANT = 16 << 20
VMEM = pl.BlockSpec(memory_space=pltpu.VMEM)
SMEM = pl.BlockSpec(memory_space=pltpu.SMEM)


def call(kernel, outs, *args, spaces, scratch=(), flops=0, moved=0):
    return pl.pallas_call(
        kernel,
        out_shape=outs,
        in_specs=spaces,
        out_specs=jax.tree.map(lambda _: VMEM, outs),
        scratch_shapes=list(scratch),
        cost_estimate=pl.CostEstimate(flops=flops, bytes_accessed=moved, transcendentals=0),
        compiler_params=pltpu.CompilerParams(vmem_limit_bytes=GRANT),
    )(*args)


def swap(x, axis, step):
    return lax.ppermute(x, axis, [(i, i ^ step) for i in range(lax.axis_size(axis))])


def density_kernel(todo, place_ref, bands_ref, table_ref, *refs):
    addend_ref, out_ref, prod_ref = refs if len(refs) == 3 else (None, *refs)
    _, _, points = bands_ref.shape
    for s in todo:
        bands = bands_ref[s].astype(jnp.float32)
        products = bands[:NVW][:, None, :] * bands[NVW:][None, :, :]
        prod_ref[s] = products.reshape(NP, points).astype(jnp.bfloat16)
    waves = table_ref.shape[1]
    tile = min(256, waves)
    for n in range(0, waves, tile):
        total = None if addend_ref is None else addend_ref[:, n : n + tile]
        for s in todo:
            at = pl.multiple_of(place_ref[s] * points, points)
            term = jnp.dot(
                prod_ref[s],
                table_ref[pl.ds(at, points), n : n + tile],
                preferred_element_type=jnp.float32,
            )
            total = term if total is None else total + term
        out_ref[:, n : n + tile] = total.astype(out_ref.dtype)


def density(places, bands, table, addend=None, final=True, todo=None):
    waves = table.shape[1]
    count, _, points = bands.shape
    todo = range(count) if todo is None else todo
    more = [] if addend is None else [addend]
    return call(
        functools.partial(density_kernel, todo),
        jax.ShapeDtypeStruct((NP, waves), jnp.bfloat16 if final else jnp.float32),
        places,
        bands,
        table,
        *more,
        spaces=[SMEM, VMEM, VMEM] + [VMEM] * len(more),
        scratch=[pltpu.VMEM((count, NP, points), jnp.bfloat16)],
        flops=2 * NP * len(todo) * points * waves,
        moved=2 * len(todo) * points * waves,
    )


def weighted_kernel(me_ref, owner_ref, transfer_ref, screened_ref, dens_ref, keep_ref, give_ref, all_ref):
    slots, share, waves = screened_ref.shape
    whole = lax.dot_general(
        screened_ref[...].reshape(slots * share, waves),
        dens_ref[...],
        (((1,), (1,)), ((), ())),
        preferred_element_type=jnp.float32,
    )
    all_ref[...] = whole.astype(jnp.bfloat16).reshape(slots, share, NP)
    me = me_ref[0]
    for s in range(slots // 2):
        to = me ^ (2 * s)
        keep_ref[s] = all_ref[owner_ref[transfer_ref[to]]]
        give_ref[s] = all_ref[owner_ref[transfer_ref[to ^ 1]]]


def block_kernel(me_row_ref, me_col_ref, dens_ref, *refs):
    count = dens_ref.shape[1] // refs[0].shape[0]
    pieces, outs, (weighted_ref, block_ref) = refs[:count], refs[count:-2], refs[-2:]
    me = me_row_ref[0]
    for s, piece in enumerate(pieces):
        share = piece.shape[0] // 2
        first = me ^ (2 * s)
        weighted_ref[pl.ds(pl.multiple_of(first * share, share), share), :] = piece[:share]
        second = first ^ 1
        weighted_ref[pl.ds(pl.multiple_of(second * share, share), share), :] = piece[share:]
    block = jnp.dot(dens_ref[...], weighted_ref[...], preferred_element_type=jnp.float32)
    block_ref[...] = (block * dens_ref.shape[1] ** (-0.5)).astype(jnp.bfloat16)
    rows = outs[0].shape[0]
    for s, out in enumerate(outs):
        at = pl.multiple_of((me_col_ref[0] ^ s) * rows, rows)
        out[...] = block_ref[pl.ds(at, rows), :]


def apply_kernel(scale, *refs):
    count = len(refs) // 2
    total = None
    for block, trial in zip(refs[:count], refs[count:-1]):
        term = jnp.dot(block[...], trial[...], preferred_element_type=jnp.float32)
        total = term if total is None else total + term
    refs[-1][...] = total * scale


def shards(
    waves_row,
    waves_col,
    window_row,
    window_col,
    plane_wave,
    screened,
    owner_slot,
    transfer_table,
    trial,
):
    rows, cols = lax.axis_size("row"), lax.axis_size("col")
    chips = rows // 2
    me_row, me_col = lax.axis_index("row"), lax.axis_index("col")
    waves, share = plane_wave.shape[1], screened.shape[1]
    steps = jnp.arange(chips, dtype=jnp.int32)

    bands = lax.dynamic_slice_in_dim(waves_col[0], window_col[0], NVW + NCW, 0)[None]
    near = me_row ^ (2 * steps)
    own = density(near, bands, plane_wave, final=False)
    step = 2
    while step < rows:
        bands = jnp.concatenate([bands, swap(bands, "row", step)])
        step *= 2
    other = swap(bands, "row", 1)
    half = density(near, bands, plane_wave, own, final=False, todo=range(1, chips))
    dens_col = density(near ^ 1, other, plane_wave, half)

    piece = jax.ShapeDtypeStruct((chips, share, NP), jnp.bfloat16)
    keep, give = call(
        weighted_kernel,
        (piece, piece),
        me_row[None],
        owner_slot,
        transfer_table[:, 0],
        screened,
        dens_col,
        spaces=[SMEM, SMEM, SMEM, VMEM, VMEM],
        scratch=[pltpu.VMEM((rows, share, NP), jnp.bfloat16)],
        flops=2 * rows * share * waves * NP,
        moved=2 * rows * share * waves,
    )
    both = jnp.concatenate([keep, swap(give, "row", 1)], axis=1)
    pieces = [both[0]] + [None] * (chips - 1)
    for s in [*range(2, chips), 1]:
        pieces[s] = swap(both[s], "row", 2 * s)

    late_waves, late_trial, _ = lax.optimization_barrier((waves_row, trial, both))
    bands_row = lax.dynamic_slice_in_dim(late_waves[0], window_row[0], NVW + NCW, 0)
    row_bands = jnp.stack([bands_row] + [swap(bands_row, "col", s) for s in range(1, cols)])
    dens_row = density(me_col ^ jnp.arange(cols, dtype=jnp.int32), row_bands, plane_wave)
    trials = [late_trial] + [swap(late_trial, "col", s) for s in range(1, cols)]

    lines = call(
        block_kernel,
        [jax.ShapeDtypeStruct((NP // cols, NP), jnp.bfloat16)] * cols,
        me_row[None],
        me_col[None],
        dens_row,
        *pieces,
        spaces=[SMEM, SMEM] + [VMEM] * (1 + chips),
        scratch=[pltpu.VMEM((waves, NP), jnp.bfloat16), pltpu.VMEM((NP, NP), jnp.bfloat16)],
        flops=2 * NP * waves * NP,
        moved=2 * waves * NP,
    )
    lines = [lines[0]] + [swap(lines[s], "col", s) for s in range(1, cols)]
    return call(
        functools.partial(apply_kernel, (cols * NP) ** (-0.5)),
        jax.ShapeDtypeStruct((NP // cols, trial.shape[1]), jnp.float32),
        *lines,
        *trials,
        spaces=[VMEM] * (2 * cols),
        flops=2 * NP * NP * trial.shape[1],
        moved=2 * cols * NP * trial.shape[1],
    )


def solution(mesh):
    return jax.shard_map(
        shards,
        mesh=mesh,
        in_specs=(
            P("row", None, "col"),
            P("col", None, "row"),
            P("row"),
            P("col"),
            P(),
            P(None, "row", None),
            P(),
            P(None, "col"),
            P("col", None),
        ),
        out_specs=P(("row", "col"), None),
        check_vma=False,
    )
```

```python
import functools

import jax
import jax.numpy as jnp
from jax import lax
from jax.experimental import pallas as pl
from jax.experimental.pallas import tpu as pltpu
from jax.sharding import PartitionSpec as P


NVW = 16
NCW = 16
NP = NVW * NCW
GRANT = 16 << 20
VMEM = pl.BlockSpec(memory_space=pltpu.VMEM)
SMEM = pl.BlockSpec(memory_space=pltpu.SMEM)


def call(kernel, outs, *args, spaces, scratch=(), flops=0, moved=0):
    return pl.pallas_call(
        kernel,
        out_shape=outs,
        in_specs=spaces,
        out_specs=jax.tree.map(lambda _: VMEM, outs),
        scratch_shapes=list(scratch),
        cost_estimate=pl.CostEstimate(flops=flops, bytes_accessed=moved, transcendentals=0),
        compiler_params=pltpu.CompilerParams(vmem_limit_bytes=GRANT),
    )(*args)


def swap(x, axis, step):
    return lax.ppermute(x, axis, [(i, i ^ step) for i in range(lax.axis_size(axis))])


def products_of(bands):
    bands = bands.astype(jnp.float32)
    products = bands[:NVW][:, None, :] * bands[NVW:][None, :, :]
    return products.reshape(NP, bands.shape[1]).astype(jnp.bfloat16)


def products_kernel(bands_ref, out_ref):
    out_ref[...] = products_of(bands_ref[0])


def products(bands):
    return call(
        products_kernel,
        jax.ShapeDtypeStruct((NP, bands.shape[2]), jnp.bfloat16),
        bands,
        spaces=[VMEM],
        flops=1 << 32,
        moved=NP * bands.shape[2],
    )


def density_kernel(todo, given, place_ref, bands_ref, table_ref, *refs):
    refs, out_ref, prod_ref = list(refs[:-2]), refs[-2], refs[-1]
    ready_ref = refs.pop(0) if given else None
    addend_ref = refs.pop(0) if refs else None
    _, _, points = bands_ref.shape
    for s in todo:
        if s or not given:
            prod_ref[s] = products_of(bands_ref[s])
    waves = table_ref.shape[1]
    tile = min(256, waves)
    for n in range(0, waves, tile):
        total = None if addend_ref is None else addend_ref[:, n : n + tile]
        for s in todo:
            at = pl.multiple_of(place_ref[s] * points, points)
            term = jnp.dot(
                prod_ref[s] if s or not given else ready_ref[...],
                table_ref[pl.ds(at, points), n : n + tile],
                preferred_element_type=jnp.float32,
            )
            total = term if total is None else total + term
        out_ref[:, n : n + tile] = total.astype(out_ref.dtype)


def density(places, bands, table, ready=None, addend=None, final=True, todo=None):
    waves = table.shape[1]
    count, _, points = bands.shape
    todo = range(count) if todo is None else todo
    more = [x for x in (ready, addend) if x is not None]
    return call(
        functools.partial(density_kernel, todo, ready is not None),
        jax.ShapeDtypeStruct((NP, waves), jnp.bfloat16 if final else jnp.float32),
        places,
        bands,
        table,
        *more,
        spaces=[SMEM, VMEM, VMEM] + [VMEM] * len(more),
        scratch=[pltpu.VMEM((count, NP, points), jnp.bfloat16)],
        flops=2 * NP * len(todo) * points * waves,
        moved=2 * len(todo) * points * waves,
    )


def weighted_kernel(flip, me_ref, owner_ref, transfer_ref, screened_ref, dens_ref, out_ref, rows_ref):
    chips, share, waves = rows_ref.shape
    me = me_ref[0] ^ flip
    for s in range(chips):
        rows_ref[s] = screened_ref[owner_ref[transfer_ref[me ^ (2 * s)]]]
    out_ref[...] = (
        lax.dot_general(
            rows_ref[...].reshape(chips * share, waves),
            dens_ref[...],
            (((1,), (1,)), ((), ())),
            preferred_element_type=jnp.float32,
        )
        .astype(jnp.bfloat16)
        .reshape(chips, share, NP)
    )


def partial_kernel(scale, me_row_ref, me_col_ref, dens_ref, trial_ref, *refs):
    count = dens_ref.shape[1] // refs[0].shape[0]
    pieces, outs, (weighted_ref, part_ref) = refs[:count], refs[count:-2], refs[-2:]
    me = me_row_ref[0]
    for s, piece in enumerate(pieces):
        share = piece.shape[0] // 2
        first = me ^ (2 * s)
        weighted_ref[pl.ds(pl.multiple_of(first * share, share), share), :] = piece[:share]
        second = first ^ 1
        weighted_ref[pl.ds(pl.multiple_of(second * share, share), share), :] = piece[share:]
    block = jnp.dot(dens_ref[...], weighted_ref[...], preferred_element_type=jnp.float32)
    block = (block * dens_ref.shape[1] ** (-0.5)).astype(jnp.bfloat16)
    part_ref[...] = jnp.dot(block, trial_ref[...], preferred_element_type=jnp.float32) * scale
    rows = outs[0].shape[0]
    for s, out in enumerate(outs):
        at = pl.multiple_of((me_col_ref[0] ^ s) * rows, rows)
        out[...] = part_ref[pl.ds(at, rows), :].astype(out.dtype)


def shards(
    waves_row,
    waves_col,
    window_row,
    window_col,
    plane_wave,
    screened,
    owner_slot,
    transfer_table,
    trial,
):
    rows, cols = lax.axis_size("row"), lax.axis_size("col")
    chips = rows // 2
    me_row, me_col = lax.axis_index("row"), lax.axis_index("col")
    waves, share = plane_wave.shape[1], screened.shape[1]
    steps = jnp.arange(chips, dtype=jnp.int32)

    def window(array, start):
        return lax.dynamic_slice_in_dim(array, start[0], NVW + NCW, 1)

    near = me_row ^ (2 * steps)
    bands = window(waves_col, window_col)
    own = products(bands)
    if rows > 2:
        bands = jnp.concatenate([bands, window(swap(waves_col, "row", 2), window_col)])
    half, step = None, 4
    while step < rows:
        done = step // 4 if step > 4 else 0
        more = {} if half is None else {"addend": half}
        half = density(
            near,
            bands,
            plane_wave,
            final=False,
            todo=range(done, step // 2),
            ready=own if half is None else None,
            **more,
        )
        bands = jnp.concatenate([bands, swap(bands, "row", step)])
        step *= 2
    other = swap(bands, "row", 1)
    half = density(
        near,
        bands,
        plane_wave,
        final=False,
        todo=range(chips // 2 if half is not None else 0, chips),
        addend=half,
        ready=own if half is None else None,
    )
    dens_col = density(near ^ 1, other, plane_wave, addend=half)

    def weighted(flip):
        return call(
            functools.partial(weighted_kernel, flip),
            jax.ShapeDtypeStruct((chips, share, NP), jnp.bfloat16),
            me_row[None],
            owner_slot,
            transfer_table[:, 0],
            screened,
            dens_col,
            spaces=[SMEM, SMEM, SMEM, VMEM, VMEM],
            scratch=[pltpu.VMEM((chips, share, waves), jnp.bfloat16)],
            flops=2 * chips * share * waves * NP,
            moved=2 * chips * share * waves,
        )

    give, keep = weighted(1), weighted(0)
    both = jnp.concatenate([keep, swap(give, "row", 1)], axis=1)
    pieces = [both[0]] + [None] * (chips - 1)
    for s in [*range(2, chips), 1]:
        pieces[s] = swap(both[s], "row", 2 * s)

    late_waves, _ = lax.optimization_barrier((waves_row, both))
    bands_row = window(late_waves, window_row)
    own_row = products(bands_row)
    row_bands = jnp.concatenate([bands_row] + [swap(bands_row, "col", s) for s in range(1, cols)])
    places = me_col ^ jnp.arange(cols, dtype=jnp.int32)
    dens_row = density(places, row_bands, plane_wave, own_row)

    vectors = trial.shape[1]
    kinds = [jnp.float32] + [jnp.bfloat16] * (cols - 1)
    parts = call(
        functools.partial(partial_kernel, (cols * NP) ** (-0.5)),
        [jax.ShapeDtypeStruct((NP // cols, vectors), kind) for kind in kinds],
        me_row[None],
        me_col[None],
        dens_row,
        trial,
        *pieces,
        spaces=[SMEM, SMEM] + [VMEM] * (2 + chips),
        scratch=[pltpu.VMEM((waves, NP), jnp.bfloat16), pltpu.VMEM((NP, vectors), jnp.float32)],
        flops=2 * NP * NP * (waves + vectors),
        moved=2 * waves * NP,
    )
    total = parts[0]
    for s in range(1, cols):
        total += swap(parts[s], "col", s).astype(jnp.float32)
    return total


def solution(mesh):
    return jax.shard_map(
        shards,
        mesh=mesh,
        in_specs=(
            P("row", None, "col"),
            P("col", None, "row"),
            P("row"),
            P("col"),
            P(),
            P(None, "row", None),
            P(),
            P(None, "col"),
            P("col", None),
        ),
        out_specs=P(("row", "col"), None),
        check_vma=False,
    )
```

```python
import functools

import jax
import jax.numpy as jnp
from jax import lax
from jax.experimental import pallas as pl
from jax.experimental.pallas import tpu as pltpu
from jax.sharding import PartitionSpec as P


NVW = 16
NCW = 16
NP = NVW * NCW
GRANT = 16 << 20
VMEM = pl.BlockSpec(memory_space=pltpu.VMEM)
ANY = pl.BlockSpec(memory_space=pl.ANY)


def call(kernel, outs, *args, spaces, scratch=(), flops=0, moved=0):
    return pl.pallas_call(
        kernel,
        out_shape=outs,
        in_specs=spaces,
        out_specs=jax.tree.map(lambda _: VMEM, outs),
        scratch_shapes=list(scratch),
        cost_estimate=pl.CostEstimate(flops=flops, bytes_accessed=moved, transcendentals=0),
        compiler_params=pltpu.CompilerParams(vmem_limit_bytes=GRANT),
    )(*args)


def swap(x, axis, step):
    return lax.ppermute(x, axis, [(i, i ^ step) for i in range(lax.axis_size(axis))])


def products_of(bands):
    bands = bands.astype(jnp.float32)
    products = bands[:NVW][:, None, :] * bands[NVW:][None, :, :]
    return products.reshape(NP, bands.shape[1]).astype(jnp.bfloat16)


def picked(which, window_ref, waves_ref):
    bands = waves_ref.shape[1]
    row = lax.broadcasted_iota(jnp.int32, (NVW + NCW, bands), 0)
    band = lax.broadcasted_iota(jnp.int32, (NVW + NCW, bands), 1)
    chooser = jnp.where(band - row == window_ref[:, which : which + 1], 1.0, 0.0).astype(jnp.bfloat16)
    return jnp.dot(chooser, waves_ref[0], preferred_element_type=jnp.float32).astype(jnp.bfloat16)


def window_kernel(which, window_ref, waves_ref, bands_ref, prod_ref):
    bands = picked(which, window_ref, waves_ref)
    bands_ref[0] = bands
    prod_ref[...] = products_of(bands)


def windowed(which, starts, array):
    points = array.shape[2]
    return call(
        functools.partial(window_kernel, which),
        [
            jax.ShapeDtypeStruct((1, NVW + NCW, points), jnp.bfloat16),
            jax.ShapeDtypeStruct((NP, points), jnp.bfloat16),
        ],
        starts,
        array,
        spaces=[VMEM] * 2,
        flops=1 << 32,
        moved=NP * points,
    )


def pair_kernel(window_ref, waves_ref, mine_ref, out_ref):
    out_ref[0] = mine_ref[0]
    out_ref[1] = picked(0, window_ref, waves_ref)


def pair(starts, array, mine):
    return call(
        pair_kernel,
        jax.ShapeDtypeStruct((2, *mine.shape[1:]), jnp.bfloat16),
        starts,
        array,
        mine,
        spaces=[VMEM] * 3,
        flops=2 * mine.size * array.shape[1],
        moved=array.size * 2,
    )


def density_kernel(todo, given, place, early, bands_ref, table_ref, *refs):
    refs, out_ref, prod_ref = list(refs[: len(refs) - 2 - early]), refs[-2], refs[-1]
    ready_ref = refs.pop(0) if given else None
    addend_ref = refs.pop(0) if refs else None
    _, _, points = bands_ref.shape
    for s in todo:
        if s or not given:
            prod_ref[s] = products_of(bands_ref[s])
    waves = table_ref.shape[1]
    tile = min(256, waves)
    starts = [pl.multiple_of(place(s) * points, points) for s in range(bands_ref.shape[0])]
    for n in range(0, waves, tile):
        total = None if addend_ref is None else addend_ref[:, n : n + tile]
        for s in todo:
            term = jnp.dot(
                prod_ref[s] if s or not given else ready_ref[...],
                table_ref[pl.ds(starts[s], points), n : n + tile],
                preferred_element_type=jnp.float32,
            )
            total = term if total is None else total + term
        out_ref[:, n : n + tile] = total.astype(out_ref.dtype)


def density(place, bands, table, ready=None, addend=None, final=True, todo=None, early=()):
    waves = table.shape[1]
    count, _, points = bands.shape
    todo = range(count) if todo is None else todo
    more = [x for x in (ready, addend) if x is not None]
    return call(
        functools.partial(density_kernel, todo, ready is not None, place, len(early)),
        jax.ShapeDtypeStruct((NP, waves), jnp.bfloat16 if final else jnp.float32),
        bands,
        table,
        *more,
        *early,
        spaces=[VMEM] * (2 + len(more)) + [ANY] * len(early),
        scratch=[pltpu.VMEM((count, NP, points), jnp.bfloat16)],
        flops=2 * NP * len(todo) * points * waves,
        moved=2 * len(todo) * points * waves,
    )


def weighted_kernel(flip, slots_ref, screened_ref, dens_ref, out_ref, rows_ref):
    chips, share, waves = rows_ref.shape
    slots = slots_ref[...]
    for s in range(chips):
        rows_ref[s] = screened_ref[slots[0, flip * chips + s]]
    out_ref[...] = (
        lax.dot_general(
            rows_ref[...].reshape(chips * share, waves),
            dens_ref[...],
            (((1,), (1,)), ((), ())),
            preferred_element_type=jnp.float32,
        )
        .astype(jnp.bfloat16)
        .reshape(chips, share, NP)
    )


def partial_kernel(scale, dens_ref, trial_ref, *refs):
    count = dens_ref.shape[1] // refs[0].shape[0]
    pieces, outs, (weighted_ref, part_ref) = refs[:count], refs[count:-2], refs[-2:]
    me = lax.axis_index("row")
    for s, piece in enumerate(pieces):
        share = piece.shape[0] // 2
        first = me ^ (2 * s)
        weighted_ref[pl.ds(pl.multiple_of(first * share, share), share), :] = piece[:share]
        second = first ^ 1
        weighted_ref[pl.ds(pl.multiple_of(second * share, share), share), :] = piece[share:]
    block = jnp.dot(dens_ref[...], weighted_ref[...], preferred_element_type=jnp.float32)
    block = (block * dens_ref.shape[1] ** (-0.5)).astype(jnp.bfloat16)
    part_ref[...] = jnp.dot(block, trial_ref[...], preferred_element_type=jnp.float32) * scale
    rows = outs[0].shape[0]
    for s, out in enumerate(outs):
        at = pl.multiple_of((lax.axis_index("col") ^ s) * rows, rows)
        out[...] = part_ref[pl.ds(at, rows), :].astype(out.dtype)


def shards(
    waves_row,
    waves_col,
    window_row,
    window_col,
    plane_wave,
    screened,
    owner_slot,
    transfer_table,
    trial,
):
    rows, cols = lax.axis_size("row"), lax.axis_size("col")
    chips = rows // 2
    waves, share = plane_wave.shape[1], screened.shape[1]

    def near(s):
        return lax.axis_index("row") ^ (2 * s)

    def across(s):
        return near(s) ^ 1

    def column(s):
        return lax.axis_index("col") ^ s

    starts = jnp.where(jnp.arange(2) == 0, window_col, window_row)[None]
    bands, own = windowed(0, starts, waves_col)
    if rows > 2:
        bands = pair(starts, swap(waves_col, "row", 2), bands)
    every = jnp.arange(rows, dtype=jnp.int32)
    order = lax.axis_index("row") ^ jnp.concatenate([every[::2], every[1::2]])
    transfers = jnp.sum(jnp.where(order[:, None] == every, transfer_table[:, 0], 0), axis=1)
    slots = jnp.sum(jnp.where(transfers[:, None] == every, owner_slot, 0), axis=1)[None]
    early = (slots,)

    half, step = None, 4
    while step < rows:
        done = step // 4 if step > 4 else 0
        more = {} if half is None else {"addend": half}
        half = density(
            near,
            bands,
            plane_wave,
            final=False,
            todo=range(done, step // 2),
            ready=own if half is None else None,
            **more,
        )
        bands = jnp.concatenate([bands, swap(bands, "row", step)])
        step *= 2
    other = swap(bands, "row", 1)
    half = density(
        near,
        bands,
        plane_wave,
        final=False,
        todo=range(chips // 2 if half is not None else 0, chips),
        addend=half,
        ready=own if half is None else None,
        early=early,
    )
    dens_col = density(across, other, plane_wave, addend=half)

    def weighted(flip):
        return call(
            functools.partial(weighted_kernel, flip),
            jax.ShapeDtypeStruct((chips, share, NP), jnp.bfloat16),
            slots,
            screened,
            dens_col,
            spaces=[VMEM] * 3,
            scratch=[pltpu.VMEM((chips, share, waves), jnp.bfloat16)],
            flops=2 * chips * share * waves * NP,
            moved=2 * chips * share * waves,
        )

    give, keep = weighted(1), weighted(0)
    both = jnp.concatenate([keep, swap(give, "row", 1)], axis=1)
    pieces = [both[0]] + [None] * (chips - 1)
    for s in [*range(2, chips), 1]:
        pieces[s] = swap(both[s], "row", 2 * s)

    late_waves, _ = lax.optimization_barrier((waves_row, both))
    bands_row, own_row = windowed(1, starts, late_waves)
    row_bands = jnp.concatenate([bands_row] + [swap(bands_row, "col", s) for s in range(1, cols)])
    dens_row = density(column, row_bands, plane_wave, own_row)

    vectors = trial.shape[1]
    kinds = [jnp.float32] + [jnp.bfloat16] * (cols - 1)
    parts = call(
        functools.partial(partial_kernel, (cols * NP) ** (-0.5)),
        [jax.ShapeDtypeStruct((NP // cols, vectors), kind) for kind in kinds],
        dens_row,
        trial,
        *pieces,
        spaces=[VMEM] * (2 + chips),
        scratch=[pltpu.VMEM((waves, NP), jnp.bfloat16), pltpu.VMEM((NP, vectors), jnp.float32)],
        flops=2 * NP * NP * (waves + vectors),
        moved=2 * waves * NP,
    )
    total = parts[0]
    for s in range(1, cols):
        total += swap(parts[s], "col", s).astype(jnp.float32)
    return total


def solution(mesh):
    return jax.shard_map(
        shards,
        mesh=mesh,
        in_specs=(
            P("row", None, "col"),
            P("col", None, "row"),
            P("row"),
            P("col"),
            P(),
            P(None, "row", None),
            P(),
            P(None, "col"),
            P("col", None),
        ),
        out_specs=P(("row", "col"), None),
        check_vma=False,
    )
```

```python
import functools

import jax
import jax.numpy as jnp
from jax import lax
from jax.experimental import pallas as pl
from jax.experimental.pallas import tpu as pltpu
from jax.sharding import PartitionSpec as P


NVW = 16
NCW = 16
NP = NVW * NCW
GRANT = 16 << 20
VMEM = pl.BlockSpec(memory_space=pltpu.VMEM)
ANY = pl.BlockSpec(memory_space=pl.ANY)


def call(kernel, outs, *args, spaces, scratch=(), flops=0, moved=0):
    return pl.pallas_call(
        kernel,
        out_shape=outs,
        in_specs=spaces,
        out_specs=jax.tree.map(lambda _: VMEM, outs),
        scratch_shapes=list(scratch),
        cost_estimate=pl.CostEstimate(flops=flops, bytes_accessed=moved, transcendentals=0),
        compiler_params=pltpu.CompilerParams(vmem_limit_bytes=GRANT),
    )(*args)


def swap(x, axis, step):
    return lax.ppermute(x, axis, [(i, i ^ step) for i in range(lax.axis_size(axis))])


def products_of(bands):
    bands = bands.astype(jnp.float32)
    products = bands[:NVW][:, None, :] * bands[NVW:][None, :, :]
    return products.reshape(NP, bands.shape[1]).astype(jnp.bfloat16)


def picked(which, window_ref, waves_ref):
    bands = waves_ref.shape[1]
    row = lax.broadcasted_iota(jnp.int32, (NVW + NCW, bands), 0)
    band = lax.broadcasted_iota(jnp.int32, (NVW + NCW, bands), 1)
    chooser = jnp.where(band - row == window_ref[:, which : which + 1], 1.0, 0.0).astype(jnp.bfloat16)
    return jnp.dot(chooser, waves_ref[0], preferred_element_type=jnp.float32).astype(jnp.bfloat16)


def window_kernel(which, window_ref, waves_ref, bands_ref, prod_ref):
    bands = picked(which, window_ref, waves_ref)
    bands_ref[0] = bands
    prod_ref[...] = products_of(bands)


def windowed(which, starts, array):
    points = array.shape[2]
    return call(
        functools.partial(window_kernel, which),
        [
            jax.ShapeDtypeStruct((1, NVW + NCW, points), jnp.bfloat16),
            jax.ShapeDtypeStruct((NP, points), jnp.bfloat16),
        ],
        starts,
        array,
        spaces=[VMEM] * 2,
        flops=1 << 32,
        moved=NP * points,
    )


def pair_kernel(window_ref, waves_ref, mine_ref, out_ref):
    out_ref[0] = mine_ref[0]
    out_ref[1] = picked(0, window_ref, waves_ref)


def pair(starts, array, mine):
    return call(
        pair_kernel,
        jax.ShapeDtypeStruct((2, *mine.shape[1:]), jnp.bfloat16),
        starts,
        array,
        mine,
        spaces=[VMEM] * 3,
        flops=2 * mine.size * array.shape[1],
        moved=array.size * 2,
    )


def density_kernel(todo, given, place, early, bands_ref, table_ref, *refs):
    refs, out_ref, prod_ref = list(refs[: len(refs) - 2 - early]), refs[-2], refs[-1]
    ready_ref = refs.pop(0) if given else None
    addend_ref = refs.pop(0) if refs else None
    _, _, points = bands_ref.shape
    for s in todo:
        if s or not given:
            prod_ref[s] = products_of(bands_ref[s])
    waves = table_ref.shape[1]
    tile = min(256, waves)
    starts = [pl.multiple_of(place(s) * points, points) for s in range(bands_ref.shape[0])]
    for n in range(0, waves, tile):
        total = None if addend_ref is None else addend_ref[:, n : n + tile]
        for s in todo:
            term = jnp.dot(
                prod_ref[s] if s or not given else ready_ref[...],
                table_ref[pl.ds(starts[s], points), n : n + tile],
                preferred_element_type=jnp.float32,
            )
            total = term if total is None else total + term
        out_ref[:, n : n + tile] = total.astype(out_ref.dtype)


def density(place, bands, table, ready=None, addend=None, final=True, todo=None, early=()):
    waves = table.shape[1]
    count, _, points = bands.shape
    todo = range(count) if todo is None else todo
    more = [x for x in (ready, addend) if x is not None]
    return call(
        functools.partial(density_kernel, todo, ready is not None, place, len(early)),
        jax.ShapeDtypeStruct((NP, waves), jnp.bfloat16 if final else jnp.float32),
        bands,
        table,
        *more,
        *early,
        spaces=[VMEM] * (2 + len(more)) + [ANY] * len(early),
        scratch=[pltpu.VMEM((count, NP, points), jnp.bfloat16)],
        flops=2 * NP * len(todo) * points * waves,
        moved=2 * len(todo) * points * waves,
    )


def weighted_kernel(picks, slots_ref, screened_ref, dens_ref, out_ref, rows_ref):
    count, share, waves = rows_ref.shape
    slots = slots_ref[...]
    for s, pick in enumerate(picks):
        rows_ref[s] = screened_ref[slots[0, pick]]
    out_ref[...] = (
        lax.dot_general(
            rows_ref[...].reshape(count * share, waves),
            dens_ref[...],
            (((1,), (1,)), ((), ())),
            preferred_element_type=jnp.float32,
        )
        .astype(jnp.bfloat16)
        .reshape(count, share, NP)
    )


def partial_kernel(scale, dens_ref, trial_ref, *refs):
    count = dens_ref.shape[1] // refs[0].shape[0]
    pieces, outs, (weighted_ref, part_ref) = refs[:count], refs[count:-2], refs[-2:]
    me = lax.axis_index("row")
    for s, piece in enumerate(pieces):
        share = piece.shape[0] // 2
        first = me ^ (2 * s)
        weighted_ref[pl.ds(pl.multiple_of(first * share, share), share), :] = piece[:share]
        second = first ^ 1
        weighted_ref[pl.ds(pl.multiple_of(second * share, share), share), :] = piece[share:]
    block = jnp.dot(dens_ref[...], weighted_ref[...], preferred_element_type=jnp.float32)
    block = (block * dens_ref.shape[1] ** (-0.5)).astype(jnp.bfloat16)
    part_ref[...] = jnp.dot(block, trial_ref[...], preferred_element_type=jnp.float32) * scale
    rows = outs[0].shape[0]
    for s, out in enumerate(outs):
        at = pl.multiple_of((lax.axis_index("col") ^ s) * rows, rows)
        out[...] = part_ref[pl.ds(at, rows), :].astype(out.dtype)


def shards(
    waves_row,
    waves_col,
    window_row,
    window_col,
    plane_wave,
    screened,
    owner_slot,
    transfer_table,
    trial,
):
    rows, cols = lax.axis_size("row"), lax.axis_size("col")
    chips = rows // 2
    waves, share = plane_wave.shape[1], screened.shape[1]

    def near(s):
        return lax.axis_index("row") ^ (2 * s)

    def across(s):
        return near(s) ^ 1

    def column(s):
        return lax.axis_index("col") ^ s

    starts = jnp.where(jnp.arange(2) == 0, window_col, window_row)[None]
    bands, own = windowed(0, starts, waves_col)
    if rows > 2:
        bands = pair(starts, swap(waves_col, "row", 2), bands)
    every = jnp.arange(rows, dtype=jnp.int32)
    order = lax.axis_index("row") ^ jnp.concatenate([every[::2], every[1::2]])
    transfers = jnp.sum(jnp.where(order[:, None] == every, transfer_table[:, 0], 0), axis=1)
    slots = jnp.sum(jnp.where(transfers[:, None] == every, owner_slot, 0), axis=1)[None]
    early = (slots, screened)

    half, step = None, 4
    while step < rows:
        done = step // 4 if step > 4 else 0
        more = {} if half is None else {"addend": half}
        half = density(
            near,
            bands,
            plane_wave,
            final=False,
            todo=range(done, step // 2),
            ready=own if half is None else None,
            **more,
        )
        bands = jnp.concatenate([bands, swap(bands, "row", step)])
        step *= 2
    other = swap(bands, "row", 1)
    half = density(
        near,
        bands,
        plane_wave,
        final=False,
        todo=range(chips // 2 if half is not None else 0, chips),
        addend=half,
        ready=own if half is None else None,
        early=early,
    )
    dens_col = density(across, other, plane_wave, addend=half)

    def weighted(picks):
        count = len(picks)
        return call(
            functools.partial(weighted_kernel, picks),
            jax.ShapeDtypeStruct((count, share, NP), jnp.bfloat16),
            slots,
            screened,
            dens_col,
            spaces=[VMEM] * 3,
            scratch=[pltpu.VMEM((count, share, waves), jnp.bfloat16)],
            flops=2 * count * share * waves * NP,
            moved=2 * count * share * waves,
        )

    far = chips // 2
    rest = [s for s in range(chips) if s != far]
    first = weighted((far, chips + far)).reshape(2 * share, NP)
    first = swap(first, "row", 2 * far)
    give = weighted([chips + s for s in rest])
    keep = weighted(rest)
    both = jnp.concatenate([keep, swap(give, "row", 1)], axis=1)
    pieces = [None] * chips
    for index, s in enumerate(rest):
        pieces[s] = swap(both[index], "row", 2 * s) if s else both[index]
    pieces[far] = jnp.concatenate([first[:share], swap(first[share:], "row", 1)])

    late_waves, _ = lax.optimization_barrier((waves_row, give))
    bands_row, own_row = windowed(1, starts, late_waves)
    row_bands = jnp.concatenate([bands_row] + [swap(bands_row, "col", s) for s in range(1, cols)])
    dens_row = density(column, row_bands, plane_wave, own_row)

    vectors = trial.shape[1]
    kinds = [jnp.float32] + [jnp.bfloat16] * (cols - 1)
    parts = call(
        functools.partial(partial_kernel, (cols * NP) ** (-0.5)),
        [jax.ShapeDtypeStruct((NP // cols, vectors), kind) for kind in kinds],
        dens_row,
        trial,
        *pieces,
        spaces=[VMEM] * (2 + chips),
        scratch=[pltpu.VMEM((waves, NP), jnp.bfloat16), pltpu.VMEM((NP, vectors), jnp.float32)],
        flops=2 * NP * NP * (waves + vectors),
        moved=2 * waves * NP,
    )
    total = parts[0]
    for s in range(1, cols):
        total += swap(parts[s], "col", s).astype(jnp.float32)
    return total


def solution(mesh):
    return jax.shard_map(
        shards,
        mesh=mesh,
        in_specs=(
            P("row", None, "col"),
            P("col", None, "row"),
            P("row"),
            P("col"),
            P(),
            P(None, "row", None),
            P(),
            P(None, "col"),
            P("col", None),
        ),
        out_specs=P(("row", "col"), None),
        check_vma=False,
    )
```

```python
import functools

import jax
import jax.numpy as jnp
from jax import lax
from jax.experimental import pallas as pl
from jax.experimental.pallas import tpu as pltpu
from jax.sharding import PartitionSpec as P


NVW = 16
NCW = 16
NP = NVW * NCW
GRANT = 16 << 20
VMEM = pl.BlockSpec(memory_space=pltpu.VMEM)
ANY = pl.BlockSpec(memory_space=pl.ANY)


def call(kernel, outs, *args, spaces, scratch=(), flops=0, moved=0):
    return pl.pallas_call(
        kernel,
        out_shape=outs,
        in_specs=spaces,
        out_specs=jax.tree.map(lambda _: VMEM, outs),
        scratch_shapes=list(scratch),
        cost_estimate=pl.CostEstimate(flops=flops, bytes_accessed=moved, transcendentals=0),
        compiler_params=pltpu.CompilerParams(vmem_limit_bytes=GRANT),
    )(*args)


def swap(x, axis, step):
    return lax.ppermute(x, axis, [(i, i ^ step) for i in range(lax.axis_size(axis))])


def products_of(bands):
    bands = bands.astype(jnp.float32)
    products = bands[:NVW][:, None, :] * bands[NVW:][None, :, :]
    return products.reshape(NP, bands.shape[1]).astype(jnp.bfloat16)


def picked(which, window_ref, waves_ref):
    bands = waves_ref.shape[1]
    row = lax.broadcasted_iota(jnp.int32, (NVW + NCW, bands), 0)
    band = lax.broadcasted_iota(jnp.int32, (NVW + NCW, bands), 1)
    chooser = jnp.where(band - row == window_ref[:, which : which + 1], 1.0, 0.0).astype(jnp.bfloat16)
    return jnp.dot(chooser, waves_ref[0], preferred_element_type=jnp.float32).astype(jnp.bfloat16)


def window_kernel(which, window_ref, waves_ref, bands_ref, prod_ref):
    bands = picked(which, window_ref, waves_ref)
    bands_ref[0] = bands
    prod_ref[...] = products_of(bands)


def windowed(which, starts, array):
    points = array.shape[2]
    return call(
        functools.partial(window_kernel, which),
        [
            jax.ShapeDtypeStruct((1, NVW + NCW, points), jnp.bfloat16),
            jax.ShapeDtypeStruct((NP, points), jnp.bfloat16),
        ],
        starts,
        array,
        spaces=[VMEM] * 2,
        flops=1 << 32,
        moved=NP * points,
    )


def pair_kernel(window_ref, waves_ref, mine_ref, out_ref):
    out_ref[0] = mine_ref[0]
    out_ref[1] = picked(0, window_ref, waves_ref)


def pair(starts, array, mine):
    return call(
        pair_kernel,
        jax.ShapeDtypeStruct((2, *mine.shape[1:]), jnp.bfloat16),
        starts,
        array,
        mine,
        spaces=[VMEM] * 3,
        flops=2 * mine.size * array.shape[1],
        moved=array.size * 2,
    )


def density_kernel(todo, given, place, early, bands_ref, table_ref, *refs):
    refs, out_ref, prod_ref = list(refs[: len(refs) - 2 - early]), refs[-2], refs[-1]
    ready_ref = refs.pop(0) if given else None
    addend_ref = refs.pop(0) if refs else None
    _, _, points = bands_ref.shape
    for s in todo:
        if s or not given:
            prod_ref[s] = products_of(bands_ref[s])
    waves = table_ref.shape[1]
    tile = min(256, waves)
    starts = [pl.multiple_of(place(s) * points, points) for s in range(bands_ref.shape[0])]
    for n in range(0, waves, tile):
        total = None if addend_ref is None else addend_ref[:, n : n + tile]
        for s in todo:
            term = jnp.dot(
                prod_ref[s] if s or not given else ready_ref[...],
                table_ref[pl.ds(starts[s], points), n : n + tile],
                preferred_element_type=jnp.float32,
            )
            total = term if total is None else total + term
        out_ref[:, n : n + tile] = total.astype(out_ref.dtype)


def density(place, bands, table, ready=None, addend=None, final=True, todo=None, early=()):
    waves = table.shape[1]
    count, _, points = bands.shape
    todo = range(count) if todo is None else todo
    more = [x for x in (ready, addend) if x is not None]
    return call(
        functools.partial(density_kernel, todo, ready is not None, place, len(early)),
        jax.ShapeDtypeStruct((NP, waves), jnp.bfloat16 if final else jnp.float32),
        bands,
        table,
        *more,
        *early,
        spaces=[VMEM] * (2 + len(more)) + [ANY] * len(early),
        scratch=[pltpu.VMEM((count, NP, points), jnp.bfloat16)],
        flops=2 * NP * len(todo) * points * waves,
        moved=2 * len(todo) * points * waves,
    )


def weighted_kernel(picks, slots_ref, screened_ref, dens_ref, out_ref, rows_ref):
    count, share, waves = rows_ref.shape
    slots = slots_ref[...]
    for s, pick in enumerate(picks):
        rows_ref[s] = screened_ref[slots[0, pick]]
    out_ref[...] = (
        lax.dot_general(
            rows_ref[...].reshape(count * share, waves),
            dens_ref[...],
            (((1,), (1,)), ((), ())),
            preferred_element_type=jnp.float32,
        )
        .astype(jnp.bfloat16)
        .reshape(count, share, NP)
    )


def partial_kernel(scale, dens_ref, trial_ref, *refs):
    count = dens_ref.shape[1] // refs[0].shape[0]
    pieces, outs, (weighted_ref, part_ref) = refs[:count], refs[count:-2], refs[-2:]
    me = lax.axis_index("row")
    for s, piece in enumerate(pieces):
        share = piece.shape[0] // 2
        first = me ^ (2 * s)
        weighted_ref[pl.ds(pl.multiple_of(first * share, share), share), :] = piece[:share]
        second = first ^ 1
        weighted_ref[pl.ds(pl.multiple_of(second * share, share), share), :] = piece[share:]
    block = jnp.dot(dens_ref[...], weighted_ref[...], preferred_element_type=jnp.float32)
    block = (block * dens_ref.shape[1] ** (-0.5)).astype(jnp.bfloat16)
    part_ref[...] = jnp.dot(block, trial_ref[...], preferred_element_type=jnp.float32) * scale
    rows = outs[0].shape[0]
    for s, out in enumerate(outs):
        at = pl.multiple_of((lax.axis_index("col") ^ s) * rows, rows)
        out[...] = part_ref[pl.ds(at, rows), :].astype(out.dtype)


def shards(
    waves_row,
    waves_col,
    window_row,
    window_col,
    plane_wave,
    screened,
    owner_slot,
    transfer_table,
    trial,
):
    rows, cols = lax.axis_size("row"), lax.axis_size("col")
    chips = rows // 2
    waves, share = plane_wave.shape[1], screened.shape[1]

    def near(s):
        return lax.axis_index("row") ^ (2 * s)

    def across(s):
        return near(s) ^ 1

    def column(s):
        return lax.axis_index("col") ^ s

    starts = jnp.where(jnp.arange(2) == 0, window_col, window_row)[None]
    bands, own = windowed(0, starts, waves_col)
    if rows > 2:
        bands = pair(starts, swap(waves_col, "row", 2), bands)
    every = jnp.arange(rows, dtype=jnp.int32)
    order = lax.axis_index("row") ^ jnp.concatenate([every[::2], every[1::2]])
    transfers = jnp.sum(jnp.where(order[:, None] == every, transfer_table[:, 0], 0), axis=1)
    slots = jnp.sum(jnp.where(transfers[:, None] == every, owner_slot, 0), axis=1)[None]
    early = (slots, screened)

    half, done, step = None, 0, 4
    while True:
        more = {"ready": own} if half is None else {"addend": half}
        todo = range(done, step // 2)
        half = density(near, bands, plane_wave, final=False, todo=todo, **more)
        if 2 * step >= rows:
            break
        bands = jnp.concatenate([bands, swap(bands, "row", step)])
        done, step = step // 2, 2 * step
    other = swap(bands, "row", 1)
    half = density(across, other, plane_wave, addend=half, final=False)
    last = swap(bands, "row", step)
    other = swap(last, "row", 1)

    def near_last(s):
        return near(s + chips // 2)

    def across_last(s):
        return across(s + chips // 2)

    half = density(near_last, last, plane_wave, addend=half, final=False, early=early)
    dens_col = density(across_last, other, plane_wave, addend=half)

    def weighted(picks):
        count = len(picks)
        return call(
            functools.partial(weighted_kernel, picks),
            jax.ShapeDtypeStruct((count, share, NP), jnp.bfloat16),
            slots,
            screened,
            dens_col,
            spaces=[VMEM] * 3,
            scratch=[pltpu.VMEM((count, share, waves), jnp.bfloat16)],
            flops=2 * count * share * waves * NP,
            moved=2 * count * share * waves,
        )

    far = chips - 1
    rest = [s for s in range(chips) if s != far]
    first = weighted((far, chips + far)).reshape(2 * share, NP)
    first = swap(first, "row", 2 * far)
    give = weighted([chips + s for s in rest])
    keep = weighted(rest)
    both = jnp.concatenate([keep, swap(give, "row", 1)], axis=1)
    pieces = [None] * chips
    for index, s in enumerate(rest):
        pieces[s] = swap(both[index], "row", 2 * s) if s else both[index]
    pieces[far] = jnp.concatenate([first[:share], swap(first[share:], "row", 1)])

    late_waves, _ = lax.optimization_barrier((waves_row, give))
    bands_row, own_row = windowed(1, starts, late_waves)
    others = [swap(bands_row, "col", s) for s in range(1, cols)]

    def other_column(s):
        return column(s + 1)

    half = density(column, bands_row, plane_wave, ready=own_row, final=False)
    dens_row = density(other_column, jnp.concatenate(others), plane_wave, addend=half)

    vectors = trial.shape[1]
    kinds = [jnp.float32] + [jnp.bfloat16] * (cols - 1)
    parts = call(
        functools.partial(partial_kernel, (cols * NP) ** (-0.5)),
        [jax.ShapeDtypeStruct((NP // cols, vectors), kind) for kind in kinds],
        dens_row,
        trial,
        *pieces,
        spaces=[VMEM] * (2 + chips),
        scratch=[pltpu.VMEM((waves, NP), jnp.bfloat16), pltpu.VMEM((NP, vectors), jnp.float32)],
        flops=2 * NP * NP * (waves + vectors),
        moved=2 * waves * NP,
    )
    total = parts[0]
    for s in range(1, cols):
        total += swap(parts[s], "col", s).astype(jnp.float32)
    return total


def solution(mesh):
    return jax.shard_map(
        shards,
        mesh=mesh,
        in_specs=(
            P("row", None, "col"),
            P("col", None, "row"),
            P("row"),
            P("col"),
            P(),
            P(None, "row", None),
            P(),
            P(None, "col"),
            P("col", None),
        ),
        out_specs=P(("row", "col"), None),
        check_vma=False,
    )
```
